32 devices in a mesh: comp: 4 (over y, x), dom: 8 (over z, core).
Axes of the slice: x: 2, y: 2, z: 4, core: 2. Of those that a mesh axis runs over, the one named last changes fastest.
Arguments:
- atm_fields: bfloat16 [24, 65536], P(None, ('comp', 'dom')), may hold values from -6 to 6
- send_cols: int32 [4, 8, 4, 4, 256], P('comp', 'dom'), may hold values from 0 to 2047
- live_blocks: int32 [4, 8, 4], P('comp', 'dom'), may hold values from 1 to 4, as said below
- remap_weights: bfloat16 [4, 8, 4, 4, 256, 256], P('comp', 'dom'), may hold values from -0.375 to 0.375
- row_map: int32 [4, 8, 4, 4, 256], P('comp', 'dom'), may hold values from 0 to 4095
- ocean_depth: float32 [256, 512], P('dom', 'comp'), may hold values from 0.25 to 8
- wet_mask: int32 [256, 512], P('dom', 'comp'), may hold values 0 or 1
- sea_level: float32 [256, 512], P('dom', 'comp'), may hold values from -3 to 3
- east_vel: float32 [256, 512], P('dom', 'comp'), may hold values from -0.3 to 0.3
- north_vel: float32 [256, 512], P('dom', 'comp'), may hold values from -0.3 to 0.3
Outputs:
- ocean_fluxes: float32 [24, 256, 512], P(None, 'dom', 'comp')
- ocean_state: float32 [3, 256, 512], P(None, 'dom', 'comp')
The draws below stay inside these ranges and needn't reach their ends.
Inputs may be any that keep to these rules, and one draw needn't show every extreme that they name: `live_blocks`: every receiving device has exactly 4 live blocks from at least one source group.
All inputs are finite; a program needn't handle non-finite values. No bound on the sum of `wet_mask` on one device may be relied on, other than what follows from the above.
Results may differ from the reference program's by a relative error of at most 0.0003.
Values may be sent and summed in bfloat16 or wider, within the bound.
A program may use at most 64 MiB of HBM per device.

```python
import jax
import jax.numpy as jnp
from jax import lax

F = 24
AC = 2048
AB = 256
OB = 256
CAP = 4
RO = 32
CO = 128
NSUB = 4
NAC = 65536
NR = 256
NCOL = 512
N_COMP = 4
N_DOM = 8


def draw_ocean_depth(key, part):
    rows_frac = jnp.arange(NR, dtype=jnp.float32)[:, None] / NR
    cols_frac = jnp.arange(NCOL, dtype=jnp.float32)[None, :] / NCOL
    trend = 0.5 * jnp.power(16.0, 0.5 * (rows_frac + cols_frac))
    rough = jnp.exp(jax.random.uniform(key, (NR, NCOL), jnp.float32, -0.69, 0.0))
    return jnp.clip(trend * rough, 0.25, 8.0)


def draw_live_blocks(key, part):
    first = jax.random.fold_in(key, 11)
    second = jax.random.fold_in(key, 23)
    base = jax.random.randint(first, (N_COMP, N_DOM, N_COMP), 1, CAP + 1)
    chosen = jax.random.randint(second, (N_COMP, N_DOM, 1), 0, N_COMP)
    source = jnp.arange(N_COMP, dtype=jnp.int32)[None, None, :]
    return jnp.where(source == chosen, CAP, base).astype(jnp.int32)


def touch_ends(array, stream_key, least, top_value):
    dims = array.shape
    place = [jax.random.randint(jax.random.fold_in(stream_key, axis), (), 0, dims[axis]) for axis in range(len(dims))]
    array = array.at[tuple(place)].set(least)
    longest = dims.index(max(dims))
    place[longest] = (place[longest] + 1) % dims[longest]
    return array.at[tuple(place)].set(top_value)


def block_levels(key, dims, split, smallest, top_value):
    def one(axis_at, parts):
        heights = jax.random.uniform(jax.random.fold_in(jax.random.fold_in(key, 6), axis_at), (parts,), jnp.float32, smallest / len(split), top_value / len(split))
        return jnp.repeat(jnp.exp(heights), dims[axis_at] // parts).reshape((-1,) + (1,) * (len(dims) - axis_at - 1))

    factor_of = one(*split[0])
    for cut in split[1:]:
        factor_of = factor_of * one(*cut)
    return factor_of


def gaussian(rng, shape, spread, reach, shards=(), held_as=jnp.bfloat16):
    values = spread * jax.random.normal(rng, shape, jnp.float32)
    if shards:
        values = values * block_levels(rng, shape, shards, -0.22, 0.18)
    return jnp.clip(values, -reach, reach).astype(held_as)


def setup_inputs(seed: int = 0) -> dict:
    streams_of = jax.random.split(jax.random.key(seed), 11)
    return {
        "atm_fields": gaussian(streams_of[0], (F, NAC), 1.0, 6.0, ((1, 32),)),
        "send_cols": touch_ends(jax.random.randint(streams_of[1], (N_COMP, N_DOM, N_COMP, CAP, AB), 0, AC), jax.random.fold_in(streams_of[1], 1), 0, AC - 1).astype(jnp.int32),
        "live_blocks": draw_live_blocks(jax.random.fold_in(streams_of[10], 71), 0),
        "remap_weights": gaussian(streams_of[3], (N_COMP, N_DOM, N_COMP, CAP, OB, AB), AB ** -0.5, 0.375, ((0, 4), (1, 8))),
        "row_map": touch_ends(jax.random.randint(streams_of[4], (N_COMP, N_DOM, N_COMP, CAP, OB), 0, RO * CO), jax.random.fold_in(streams_of[4], 1), 0, (RO * CO) - 1).astype(jnp.int32),
        "ocean_depth": draw_ocean_depth(jax.random.fold_in(streams_of[10], 71), 0),
        "wet_mask": touch_ends((jax.random.randint(streams_of[6], (NR, NCOL), 0, 10) < 9).astype(jnp.int32), jax.random.fold_in(streams_of[6], 1), 0, 1),
        "sea_level": gaussian(streams_of[7], (NR, NCOL), 0.5, 3.0, ((0, 8), (1, 4)), jnp.float32),
        "east_vel": gaussian(streams_of[8], (NR, NCOL), 0.1, 0.3, ((0, 8), (1, 4)), jnp.float32),
        "north_vel": gaussian(streams_of[9], (NR, NCOL), 0.1, 0.3, ((0, 8), (1, 4)), jnp.float32),
    }


courant = 0.5
friction = 0.05

def level_update(level, flux_x, flux_y, fresh, wetness, step_dt):
    diverge = 0.5 * (flux_x[1:-1, 2:] - flux_x[1:-1, :-2] + (flux_y[2:, 1:-1] - flux_y[:-2, 1:-1]))
    return wetness[1:-1, 1:-1] * (level[1:-1, 1:-1] + step_dt * (fresh[1:-1, 1:-1] - diverge))

def velocity_update(east, north, level_ext, rotation, push_x, push_y, wetness, step_dt):
    grad_x = 0.5 * (level_ext[1:-1, 2:] - level_ext[1:-1, :-2])
    grad_y = 0.5 * (level_ext[2:, 1:-1] - level_ext[:-2, 1:-1])
    new_east = wetness * (east + step_dt * (rotation * north - grad_x + push_x - friction * east))
    new_north = wetness * (north + step_dt * (-rotation * east - grad_y + push_y - friction * north))
    return (new_east, new_north)

def reference(atm_fields, send_cols, live_blocks, remap_weights, row_map, ocean_depth, wet_mask, sea_level, east_vel, north_vel):
    fields = atm_fields.reshape(F, N_COMP, N_DOM, AC)
    slots = jnp.arange(CAP, dtype=jnp.int32)

    def one_device(index):
        group = index // N_DOM
        part_d = index % N_DOM
        cols = send_cols[:, part_d, group]
        sources = jnp.transpose(fields[:, :, part_d, :], (1, 0, 2))
        blocks = jax.vmap(lambda source, column: jnp.take(source, column.reshape(-1), axis=1).reshape(F, CAP, AB))(sources, cols)
        weights = remap_weights[group, part_d]
        contrib = jnp.einsum('sfkb,skob->skfo', blocks.astype(jnp.float32), weights.astype(jnp.float32))
        alive = (slots[None, :] < live_blocks[group, part_d][:, None]).astype(jnp.float32)
        contrib = contrib * alive[:, :, None, None]
        flat = jnp.transpose(contrib, (2, 0, 1, 3)).reshape(F, -1)
        total = jnp.zeros((F, RO * CO), jnp.float32).at[:, row_map[group, part_d].reshape(-1)].add(flat)
        return total.reshape(F, RO, CO)
    blocks_out = lax.map(one_device, jnp.arange(N_COMP * N_DOM, dtype=jnp.int32))
    fluxes = blocks_out.reshape(N_COMP, N_DOM, F, RO, CO)
    fluxes = jnp.transpose(fluxes, (2, 1, 3, 0, 4)).reshape(F, NR, NCOL)
    wetness = wet_mask.astype(jnp.float32)
    push_x = fluxes[0] / ocean_depth
    push_y = fluxes[1] / ocean_depth
    fresh = fluxes[2]
    rows_idx = jnp.arange(NR, dtype=jnp.float32)
    rotation = (0.1 + 0.4 * (rows_idx + 0.5) / NR)[:, None]

    def padded(value):
        return jnp.pad(value, 1)
    level, east, north = (sea_level, east_vel, north_vel)
    for substep in range(NSUB):
        speed = jnp.sqrt(ocean_depth) + wetness * (jnp.abs(east) + jnp.abs(north))
        step_dt = courant / jnp.max(speed)
        flux_x = ocean_depth * east * wetness
        flux_y = ocean_depth * north * wetness
        new_level = level_update(padded(level), padded(flux_x), padded(flux_y), padded(fresh), padded(wetness), step_dt)
        east, north = velocity_update(east, north, padded(new_level), rotation, push_x, push_y, wetness, step_dt)
        level = new_level
    return (fluxes, jnp.stack([level, east, north]))
```

```python
import functools

import jax
import jax.numpy as jnp
from jax import lax
from jax.experimental import pallas as pl
from jax.experimental.pallas import tpu as pltpu
from jax.sharding import PartitionSpec as P

NSUB = 4
HALO = 2 * NSUB
LANES = 128

courant = 0.5
friction = 0.05

MESH = pl.DeviceIdType.MESH
COMPASS = [(-1, 0), (1, 0), (0, 1), (0, -1), (1, 1), (-1, 1), (1, -1), (-1, -1)]


def nt_dot(a, b):
    return lax.dot_general(a, b, (((1,), (1,)), ((), ())), preferred_element_type=jnp.float32)


def log2(n):
    assert n & (n - 1) == 0
    return n.bit_length() - 1


def pack_edges(fields):
    slot = lax.broadcasted_iota(jnp.int32, fields[0].shape, 1) // (2 * HALO)
    packed = jnp.zeros_like(fields[0])
    for i, field in enumerate(fields):
        packed = jnp.where(slot == i, pltpu.roll(field, 2 * HALO * i + HALO, 1), packed)
    return packed


def gather_kernel(
    atm_ref, cols_ref, live_ref, map_ref, depth_ref, wet_ref, level_ref, east_ref, north_ref,
    out_ref, target_ref, init_ref, edges_ref, speed_ref, wide,
):
    nfield, ncol = atm_ref.shape
    ngroup, capacity, width = cols_ref.shape
    dead = depth_ref.shape[0] * depth_ref.shape[1]
    wide[...] = atm_ref[...].astype(jnp.float32)

    wet = wet_ref[...].astype(jnp.float32)
    fields = [level_ref[...], east_ref[...], north_ref[...], depth_ref[...], wet]
    for i, field in enumerate(fields):
        init_ref[i] = field
    edges_ref[...] = pack_edges(fields)
    speed = jnp.sqrt(fields[3]) + wet * (jnp.abs(fields[1]) + jnp.abs(fields[2]))
    speed_ref[...] = jnp.max(speed, axis=0, keepdims=True)

    slot = lax.broadcasted_iota(jnp.int32, (capacity, width), 0)
    for s in range(ngroup):
        target_ref[s] = jnp.where(slot < live_ref[s], map_ref[s], dead)

    def group(g, carry):
        lists = cols_ref[g]
        for part in range(width // LANES):
            rows = []
            for k in range(capacity):
                index = lists[k : k + 1, part * LANES : (part + 1) * LANES]
                index = jnp.broadcast_to(index, (nfield, LANES))
                high = index >> log2(LANES)
                low = index & (LANES - 1)
                value = jnp.zeros((nfield, LANES), jnp.float32)
                for c in range(ncol // LANES):
                    chunk = wide[:, c * LANES : (c + 1) * LANES]
                    taken = jnp.take_along_axis(chunk, low, axis=1, mode="promise_in_bounds")
                    value = jnp.where(high == c, taken, value)
                rows.append(value)
            out_ref[g, :, part * LANES : (part + 1) * LANES] = jnp.concatenate(rows, 0).astype(
                out_ref.dtype
            )
        return carry

    lax.fori_loop(0, ngroup, group, 0)


def ocean_kernel(
    nc, nd,
    blocks_ref, target_ref, init_ref, edges_ref, speed_ref, weights_hbm,
    flux_hbm, state_ref,
    weights, arrived, contrib, acc, flux, push_edges, rows_in, side_in, push_rows_in, push_side_in,
    fast, fastest,
    weight_sem, flux_sem, block_send, block_recv, halo_send, halo_recv, fast_send, fast_recv,
):
    me_c, me_d = lax.axis_index("comp"), lax.axis_index("dom")
    nfield, nrows, ncols = flux.shape
    capacity, width = target_ref.shape[1:]
    half = nrows // 2
    total = nc * nd

    def weight_copy(offset):
        source = lax.rem(me_c + nc - offset, nc)
        return pltpu.make_async_copy(
            weights_hbm.at[source], weights.at[offset], weight_sem.at[offset]
        )

    def others(act):
        for dc in range(nc):
            c = lax.rem(me_c + dc, nc)

            def one(dd, carry, dc=dc, c=c):
                d = lax.rem(me_d + dd, nd)
                act(dc * nd + dd - 1, (c, d))
                return carry

            lax.fori_loop(1 if dc == 0 else 0, nd, one, 0)

    barrier = pltpu.get_barrier_semaphore()
    others(
        lambda slot, device: pl.semaphore_signal(
            barrier, inc=1, device_id=device, device_id_type=MESH
        )
    )
    for offset in range(nc):
        weight_copy(offset).start()

    def send_fast(turn, src):
        def act(slot, device):
            pltpu.make_async_remote_copy(
                src_ref=src,
                dst_ref=fastest.at[turn, slot],
                send_sem=fast_send.at[turn],
                recv_sem=fast_recv.at[turn],
                device_id=device,
                device_id_type=MESH,
            ).start()

        others(act)

    def wait_fast(turn):
        pltpu.make_async_copy(fastest.at[turn], fastest.at[turn], fast_recv.at[turn]).wait()

    def halo_refs(step, rows, edges, rows_into, side_into):
        dr, dc = step
        side = (0 if dc > 0 else 1) if dc else (0 if dr > 0 else 1)
        near = pl.ds(nrows - HALO, HALO) if dr > 0 else pl.ds(0, HALO)
        if dc == 0:
            return rows.at[:, near, :], rows_into.at[side]
        if dr == 0:
            return edges, side_into.at[side, pl.ds(HALO, nrows), :]
        far = pl.ds(0, HALO) if dr > 0 else pl.ds(HALO + nrows, HALO)
        return edges.at[near, :], side_into.at[side, far, :]

    def inside(c, d):
        return (c >= 0) & (c < nc) & (d >= 0) & (d < nd)

    def send_halo(turn, *refs):
        for i, step in enumerate(COMPASS):
            src, dst = halo_refs(step, *refs)
            c, d = me_c + step[1], me_d + step[0]

            @pl.when(inside(c, d))
            def _(i=i, src=src, dst=dst, c=c, d=d):
                pltpu.make_async_remote_copy(
                    src_ref=src,
                    dst_ref=dst,
                    send_sem=halo_send.at[turn, i],
                    recv_sem=halo_recv.at[turn, i],
                    device_id=(c, d),
                    device_id_type=MESH,
                ).start()

    def clear_halo(*refs):
        for step in COMPASS:
            _, dst = halo_refs(step, *refs)

            @pl.when(jnp.logical_not(inside(me_c - step[1], me_d - step[0])))
            def _(dst=dst):
                dst[...] = jnp.zeros(dst.shape, dst.dtype)

    def wait_halo(turn, *refs):
        for i, step in enumerate(COMPASS):
            _, dst = halo_refs(step, *refs)

            @pl.when(inside(me_c - step[1], me_d - step[0]))
            def _(i=i, dst=dst):
                pltpu.make_async_copy(dst, dst, halo_recv.at[turn, i]).wait()

    def drain_halo(turn, *refs):
        for i, step in enumerate(COMPASS):
            src, _ = halo_refs(step, *refs)

            @pl.when(inside(me_c + step[1], me_d + step[0]))
            def _(i=i, src=src):
                pltpu.make_async_copy(src, src, halo_send.at[turn, i]).wait()

    def block_copy(offset):
        peer = lax.rem(me_c + offset, nc)
        return pltpu.make_async_remote_copy(
            src_ref=blocks_ref.at[peer],
            dst_ref=arrived.at[offset - 1],
            send_sem=block_send.at[offset - 1],
            recv_sem=block_recv.at[offset - 1],
            device_id=(peer, me_d),
            device_id_type=MESH,
        )

    key_iota = lax.broadcasted_iota(jnp.int32, (2 * ncols, width), 0)
    row_iota = lax.broadcasted_iota(jnp.int32, (half, width), 0)

    def deposit(offset):
        source = lax.rem(me_c + nc - offset, nc)
        blocks = blocks_ref[source] if offset == 0 else arrived[offset - 1]
        for k in range(capacity):
            product = nt_dot(blocks, weights[offset, k])
            contrib[k] = product[k * nfield : (k + 1) * nfield]

        targets = target_ref[source]
        for k in range(capacity):
            target = targets[k : k + 1, :]
            row = target >> log2(ncols)
            key = ((row >> log2(half)) << log2(ncols)) + (target & (ncols - 1))
            group = row & (half - 1)
            chosen = jnp.where(key_iota == key, 1.0, 0.0).astype(jnp.bfloat16)
            where_row = jnp.where(row_iota == group, 1.0, 0.0)
            spread = (contrib[k][:, None, :] * where_row[None]).reshape(nfield * half, width)
            top = spread.astype(jnp.bfloat16)
            rest = (spread - top.astype(jnp.float32)).astype(jnp.bfloat16)
            update = nt_dot(top, chosen) + nt_dot(rest, chosen)
            if offset == 0 and k == 0:
                acc[...] = update
            else:
                acc[...] += update

    first = (init_ref, edges_ref, rows_in, side_in)
    second = (flux.at[pl.ds(0, 3)], push_edges, push_rows_in, push_side_in)
    clear_halo(*first)
    clear_halo(*second)
    weight_copy(0).wait()
    deposit(0)

    pl.semaphore_wait(barrier, total - 1)
    for offset in range(1, nc):
        block_copy(offset).start()
    send_halo(0, *first)
    send_fast(0, speed_ref)

    for offset in range(1, nc):
        weight_copy(offset).wait()
        block_copy(offset).wait_recv()
        deposit(offset)

    pushes = []
    for f in range(nfield):
        upper = acc[f * half : (f + 1) * half, :ncols]
        lower = acc[f * half : (f + 1) * half, ncols:]
        flux[f, :half] = upper
        flux[f, half:] = lower
        if f < 3:
            pushes.append(jnp.concatenate([upper, lower], 0))
        if f == 2:
            push_edges[...] = pack_edges(pushes)
    send_halo(1, *second)
    flux_copy = pltpu.make_async_copy(flux, flux_hbm, flux_sem)
    flux_copy.start()

    high = nrows + 2 * HALO
    lane = lax.broadcasted_iota(jnp.int32, (high, ncols), 1)
    beside = (lane < HALO) | (lane >= ncols - HALO)
    west_part = (lane & (2 * HALO - 1)) < HALO

    def extended(i, center, rows, mixed):
        main = jnp.concatenate([rows[0, i], center, rows[1, i]], 0)
        side = pltpu.roll(mixed, ncols - (2 * HALO * i + HALO), 1)
        return jnp.concatenate([main, jnp.where(beside, side, 0.0)], 1)

    wait_halo(0, *first)
    mixed = jnp.where(west_part, side_in[0], side_in[1])
    level, east, north, depth, wet = [
        extended(i, init_ref[i], rows_in, mixed) for i in range(5)
    ]
    root_depth = jnp.sqrt(init_ref[3])
    wet_here = init_ref[4]
    conduct = depth * wet
    some_depth = jnp.where(depth > 0.0, depth, 1.0)
    global_row = (
        lax.broadcasted_iota(jnp.int32, (high, 2 * ncols), 0) + (me_d * nrows - HALO)
    ).astype(jnp.float32)
    rotation = 0.1 + 0.4 * (global_row + 0.5) / (nrows * nd)

    def across(x):
        return pltpu.roll(x, 2 * ncols - 1, 1) - pltpu.roll(x, 1, 1)

    def along(x):
        return pltpu.roll(x, high - 1, 0) - pltpu.roll(x, 1, 0)

    wait_halo(1, *second)
    mixed = jnp.where(west_part, push_side_in[0], push_side_in[1])
    push_x, push_y, fresh = [
        extended(i, flux[i], push_rows_in, mixed) for i in range(3)
    ]
    push_x = push_x / some_depth
    push_y = push_y / some_depth

    for turn in range(NSUB):
        own = speed_ref if turn == 0 else fast.at[turn - 1]
        diverge = 0.5 * (across(conduct * east) + along(conduct * north))
        wait_fast(turn)
        peak = jnp.maximum(jnp.max(fastest[turn], axis=0), own[...])
        step_dt = courant / jnp.max(peak, axis=1, keepdims=True)
        level = wet * (level + step_dt * (fresh - diverge))
        east, north = (
            wet * (east + step_dt * (rotation * north - 0.5 * across(level) + push_x - friction * east)),
            wet * (north + step_dt * (-rotation * east - 0.5 * along(level) + push_y - friction * north)),
        )
        if turn < NSUB - 1:
            near_east = east[HALO : HALO + nrows, :ncols]
            near_north = north[HALO : HALO + nrows, :ncols]
            speed = root_depth + wet_here * (jnp.abs(near_east) + jnp.abs(near_north))
            fast[turn] = jnp.max(speed, axis=0, keepdims=True)
            send_fast(turn + 1, fast.at[turn])

    for i, value in enumerate((level, east, north)):
        state_ref[i] = value[HALO : HALO + nrows, :ncols]

    for offset in range(1, nc):
        block_copy(offset).wait_send()
    drain_halo(0, *first)
    drain_halo(1, *second)
    for turn in range(NSUB):
        pltpu.make_async_copy(fastest.at[turn], fastest.at[turn], fast_send.at[turn]).wait()
    flux_copy.wait()


def shards(
    nc, nd,
    atm_fields, send_cols, live_blocks, remap_weights, row_map,
    ocean_depth, wet_mask, sea_level, east_vel, north_vel,
):
    nfield, ncol = atm_fields.shape
    ngroup, capacity, width = send_cols.shape[2:]
    nrows, ncols = ocean_depth.shape
    f32, bf16 = jnp.float32, jnp.bfloat16
    vmem = pl.BlockSpec(memory_space=pltpu.VMEM)
    smem = pl.BlockSpec(memory_space=pltpu.SMEM)
    anywhere = pl.BlockSpec(memory_space=pl.ANY)

    blocks, targets, init, edges, speed = pl.pallas_call(
        gather_kernel,
        name="gather_columns",
        out_shape=(
            jax.ShapeDtypeStruct((ngroup, capacity * nfield, width), bf16),
            jax.ShapeDtypeStruct((ngroup, capacity, width), jnp.int32),
            jax.ShapeDtypeStruct((5, nrows, ncols), f32),
            jax.ShapeDtypeStruct((nrows, ncols), f32),
            jax.ShapeDtypeStruct((1, ncols), f32),
        ),
        in_specs=[vmem, vmem, smem] + [vmem] * 6,
        out_specs=[vmem] * 5,
        scratch_shapes=[pltpu.VMEM((nfield, ncol), f32)],
    )(
        atm_fields, send_cols[0, 0], live_blocks[0, 0], row_map[0, 0],
        ocean_depth, wet_mask, sea_level, east_vel, north_vel,
    )

    high = nrows + 2 * HALO
    dma = pltpu.SemaphoreType.DMA
    fluxes, state = pl.pallas_call(
        functools.partial(ocean_kernel, nc, nd),
        name="remap_and_step",
        out_shape=(
            jax.ShapeDtypeStruct((nfield, nrows, ncols), f32),
            jax.ShapeDtypeStruct((3, nrows, ncols), f32),
        ),
        in_specs=[vmem] * 5 + [anywhere],
        out_specs=[anywhere, vmem],
        scratch_shapes=[
            pltpu.VMEM((nc, capacity, width, width), bf16),
            pltpu.VMEM((nc - 1, capacity * nfield, width), bf16),
            pltpu.VMEM((capacity, nfield, width), f32),
            pltpu.VMEM((nfield * nrows // 2, 2 * ncols), f32),
            pltpu.VMEM((nfield, nrows, ncols), f32),
            pltpu.VMEM((nrows, ncols), f32),
            pltpu.VMEM((2, 5, HALO, ncols), f32),
            pltpu.VMEM((2, high, ncols), f32),
            pltpu.VMEM((2, 3, HALO, ncols), f32),
            pltpu.VMEM((2, high, ncols), f32),
            pltpu.VMEM((NSUB - 1, 1, ncols), f32),
            pltpu.VMEM((NSUB, nc * nd - 1, 1, ncols), f32),
            dma((nc,)),
            dma(()),
            dma((nc - 1,)),
            dma((nc - 1,)),
            dma((2, 8)),
            dma((2, 8)),
            dma((NSUB,)),
            dma((NSUB,)),
        ],
        compiler_params=pltpu.CompilerParams(collective_id=0, has_side_effects=True),
    )(blocks, targets, init, edges, speed, remap_weights[0, 0])
    return fluxes, state


def solution(mesh):
    in_specs = (
        P(None, ("comp", "dom")),
        P("comp", "dom", None, None, None),
        P("comp", "dom", None),
        P("comp", "dom", None, None, None, None),
        P("comp", "dom", None, None, None),
        P("dom", "comp"),
        P("dom", "comp"),
        P("dom", "comp"),
        P("dom", "comp"),
        P("dom", "comp"),
    )
    out_specs = (P(None, "dom", "comp"), P(None, "dom", "comp"))
    body = functools.partial(shards, mesh.shape["comp"], mesh.shape["dom"])
    return jax.shard_map(body, mesh=mesh, in_specs=in_specs, out_specs=out_specs, check_vma=False)
```

```python
import functools

import jax
import jax.numpy as jnp
from jax import lax
from jax.experimental import pallas as pl
from jax.experimental.pallas import tpu as pltpu
from jax.sharding import PartitionSpec as P

NSUB = 4
HALO = 2 * NSUB
LANES = 128

courant = 0.5
friction = 0.05

MESH = pl.DeviceIdType.MESH
COMPASS = [(-1, 0), (1, 0), (0, 1), (0, -1), (1, 1), (-1, 1), (1, -1), (-1, -1)]


def nt_dot(a, b):
    return lax.dot_general(a, b, (((1,), (1,)), ((), ())), preferred_element_type=jnp.float32)


def log2(n):
    assert n & (n - 1) == 0
    return n.bit_length() - 1


def pack_edges(fields):
    slot = lax.broadcasted_iota(jnp.int32, fields[0].shape, 1) // (2 * HALO)
    packed = jnp.zeros_like(fields[0])
    for i, field in enumerate(fields):
        packed = jnp.where(slot == i, pltpu.roll(field, 2 * HALO * i + HALO, 1), packed)
    return packed


def write_out(flux_ref, state_ref, flux_out, state_out, sems):
    copies = [
        pltpu.make_async_copy(flux_ref, flux_out, sems.at[0]),
        pltpu.make_async_copy(state_ref, state_out, sems.at[1]),
    ]
    for copy in copies:
        copy.start()
    for copy in copies:
        copy.wait()


def ocean_kernel(
    nc, nd,
    atm_ref, cols_ref, live_ref, map_ref, depth_ref, wet_ref, level_ref, east_ref, north_ref,
    weights_hbm,
    flux, state_ref,
    wide, blocks_ref, target_ref, init_ref, edges_ref, speed_ref,
    weights, arrived, acc, push_edges, rows_in, side_in, push_rows_in, push_side_in,
    fast, fastest,
    weight_sem, block_send, block_recv, halo_send, halo_recv, fast_send, fast_recv,
):
    me_c, me_d = lax.axis_index("comp"), lax.axis_index("dom")
    nfield, nrows, ncols = flux.shape
    capacity, width = target_ref.shape[1:]
    half = nrows // 2
    total = nc * nd

    def weight_copy(offset):
        source = lax.rem(me_c + nc - offset, nc)
        return pltpu.make_async_copy(
            weights_hbm.at[source], weights.at[offset], weight_sem.at[offset]
        )

    def others(act):
        for dc in range(nc):
            c = lax.rem(me_c + dc, nc)

            def one(dd, carry, dc=dc, c=c):
                d = lax.rem(me_d + dd, nd)
                act(dc * nd + dd - 1, (c, d))
                return carry

            lax.fori_loop(1 if dc == 0 else 0, nd, one, 0)

    barrier = pltpu.get_barrier_semaphore()
    others(
        lambda slot, device: pl.semaphore_signal(
            barrier, inc=1, device_id=device, device_id_type=MESH
        )
    )
    for offset in range(nc):
        weight_copy(offset).start()

    def send_fast(turn, src):
        def act(slot, device):
            pltpu.make_async_remote_copy(
                src_ref=src,
                dst_ref=fastest.at[turn, slot],
                send_sem=fast_send.at[turn],
                recv_sem=fast_recv.at[turn],
                device_id=device,
                device_id_type=MESH,
            ).start()

        others(act)

    def wait_fast(turn):
        pltpu.make_async_copy(fastest.at[turn], fastest.at[turn], fast_recv.at[turn]).wait()

    def halo_refs(step, rows, edges, rows_into, side_into):
        dr, dc = step
        side = (0 if dc > 0 else 1) if dc else (0 if dr > 0 else 1)
        near = pl.ds(nrows - HALO, HALO) if dr > 0 else pl.ds(0, HALO)
        if dc == 0:
            return rows.at[:, near, :], rows_into.at[side]
        if dr == 0:
            return edges, side_into.at[side, pl.ds(HALO, nrows), :]
        far = pl.ds(0, HALO) if dr > 0 else pl.ds(HALO + nrows, HALO)
        return edges.at[near, :], side_into.at[side, far, :]

    def inside(c, d):
        return (c >= 0) & (c < nc) & (d >= 0) & (d < nd)

    def send_halo(turn, *refs):
        for i, step in enumerate(COMPASS):
            src, dst = halo_refs(step, *refs)
            c, d = me_c + step[1], me_d + step[0]

            @pl.when(inside(c, d))
            def _(i=i, src=src, dst=dst, c=c, d=d):
                pltpu.make_async_remote_copy(
                    src_ref=src,
                    dst_ref=dst,
                    send_sem=halo_send.at[turn, i],
                    recv_sem=halo_recv.at[turn, i],
                    device_id=(c, d),
                    device_id_type=MESH,
                ).start()

    def clear_halo(*refs):
        for step in COMPASS:
            _, dst = halo_refs(step, *refs)

            @pl.when(jnp.logical_not(inside(me_c - step[1], me_d - step[0])))
            def _(dst=dst):
                dst[...] = jnp.zeros(dst.shape, dst.dtype)

    def wait_halo(turn, *refs):
        for i, step in enumerate(COMPASS):
            _, dst = halo_refs(step, *refs)

            @pl.when(inside(me_c - step[1], me_d - step[0]))
            def _(i=i, dst=dst):
                pltpu.make_async_copy(dst, dst, halo_recv.at[turn, i]).wait()

    def drain_halo(turn, *refs):
        for i, step in enumerate(COMPASS):
            src, _ = halo_refs(step, *refs)

            @pl.when(inside(me_c + step[1], me_d + step[0]))
            def _(i=i, src=src):
                pltpu.make_async_copy(src, src, halo_send.at[turn, i]).wait()

    def block_copy(offset):
        peer = lax.rem(me_c + offset, nc)
        return pltpu.make_async_remote_copy(
            src_ref=blocks_ref.at[offset],
            dst_ref=arrived.at[offset - 1],
            send_sem=block_send.at[offset - 1],
            recv_sem=block_recv.at[offset - 1],
            device_id=(peer, me_d),
            device_id_type=MESH,
        )

    wide[...] = atm_ref[...].astype(jnp.float32)
    wetness = wet_ref[...].astype(jnp.float32)
    fields = [level_ref[...], east_ref[...], north_ref[...], depth_ref[...], wetness]
    for i, field in enumerate(fields):
        init_ref[i] = field
    edges_ref[...] = pack_edges(fields)
    speed = jnp.sqrt(fields[3]) + wetness * (jnp.abs(fields[1]) + jnp.abs(fields[2]))
    speed_ref[...] = jnp.max(speed, axis=0, keepdims=True)

    slot = lax.broadcasted_iota(jnp.int32, (capacity, width), 0)
    for s in range(nc):
        target_ref[s] = jnp.where(slot < live_ref[s], map_ref[s], nrows * ncols)

    def gather(offset, carry):
        lists = cols_ref[lax.rem(me_c + offset, nc)]
        for part in range(width // LANES):
            picked = []
            for k in range(capacity):
                index = lists[k : k + 1, part * LANES : (part + 1) * LANES]
                index = jnp.broadcast_to(index, (nfield, LANES))
                high_bits = index >> log2(LANES)
                low_bits = index & (LANES - 1)
                value = jnp.zeros((nfield, LANES), jnp.float32)
                for c in range(wide.shape[1] // LANES):
                    chunk = wide[:, c * LANES : (c + 1) * LANES]
                    taken = jnp.take_along_axis(chunk, low_bits, axis=1, mode="promise_in_bounds")
                    value = jnp.where(high_bits == c, taken, value)
                picked.append(value)
            blocks_ref[offset, :, part * LANES : (part + 1) * LANES] = jnp.concatenate(
                picked, 0
            ).astype(blocks_ref.dtype)
        return carry

    key_iota = lax.broadcasted_iota(jnp.int32, (2 * ncols, width), 0)
    row_iota = lax.broadcasted_iota(jnp.int32, (half, width), 0)

    def deposit(offset):
        source = lax.rem(me_c + nc - offset, nc)
        blocks = blocks_ref[0] if offset == 0 else arrived[offset - 1]
        targets = target_ref[source]
        tops, rests, keys = [], [], []
        for k in range(capacity):
            product = nt_dot(blocks, weights[offset, k])[k * nfield : (k + 1) * nfield]
            target = targets[k : k + 1, :]
            row = target >> log2(ncols)
            key = ((row >> log2(half)) << log2(ncols)) + (target & (ncols - 1))
            group = row & (half - 1)
            keys.append(jnp.where(key_iota == key, 1.0, 0.0).astype(jnp.bfloat16))
            where_row = jnp.where(row_iota == group, 1.0, 0.0)
            spread = (product[:, None, :] * where_row[None]).reshape(nfield * half, width)
            tops.append(spread.astype(jnp.bfloat16))
            rests.append((spread - tops[-1].astype(jnp.float32)).astype(jnp.bfloat16))
        update = nt_dot(jnp.concatenate(tops + rests, 1), jnp.concatenate(keys + keys, 1))
        if offset == 0:
            acc[...] = update
        else:
            acc[...] += update

    first = (init_ref, edges_ref, rows_in, side_in)
    second = (flux.at[pl.ds(0, 3)], push_edges, push_rows_in, push_side_in)
    clear_halo(*first)
    clear_halo(*second)
    lax.fori_loop(0, nc, gather, 0)

    pl.semaphore_wait(barrier, total - 1)
    for offset in range(1, nc):
        block_copy(offset).start()
    send_halo(0, *first)
    send_fast(0, speed_ref)

    for offset in range(nc):
        weight_copy(offset).wait()
        if offset:
            block_copy(offset).wait_recv()
        deposit(offset)

    pushes = []
    for f in range(nfield):
        upper = acc[f * half : (f + 1) * half, :ncols]
        lower = acc[f * half : (f + 1) * half, ncols:]
        flux[f, :half] = upper
        flux[f, half:] = lower
        if f < 3:
            pushes.append(jnp.concatenate([upper, lower], 0))
        if f == 2:
            push_edges[...] = pack_edges(pushes)
    send_halo(1, *second)

    high = nrows + 2 * HALO
    lane = lax.broadcasted_iota(jnp.int32, (high, ncols), 1)
    beside = (lane < HALO) | (lane >= ncols - HALO)
    west_part = (lane & (2 * HALO - 1)) < HALO

    def extended(i, center, rows, mixed):
        main = jnp.concatenate([rows[0, i], center, rows[1, i]], 0)
        side = pltpu.roll(mixed, ncols - (2 * HALO * i + HALO), 1)
        return jnp.concatenate([main, jnp.where(beside, side, 0.0)], 1)

    wait_halo(0, *first)
    mixed = jnp.where(west_part, side_in[0], side_in[1])
    level, east, north, depth, wet = [
        extended(i, init_ref[i], rows_in, mixed) for i in range(5)
    ]
    root_depth = jnp.sqrt(init_ref[3])
    wet_here = init_ref[4]
    conduct = depth * wet
    some_depth = jnp.where(depth > 0.0, depth, 1.0)
    global_row = (
        lax.broadcasted_iota(jnp.int32, (high, 2 * ncols), 0) + (me_d * nrows - HALO)
    ).astype(jnp.float32)
    rotation = 0.1 + 0.4 * (global_row + 0.5) / (nrows * nd)

    def across(x):
        return pltpu.roll(x, 2 * ncols - 1, 1) - pltpu.roll(x, 1, 1)

    def along(x):
        return pltpu.roll(x, high - 1, 0) - pltpu.roll(x, 1, 0)

    wait_halo(1, *second)
    mixed = jnp.where(west_part, push_side_in[0], push_side_in[1])
    push_x, push_y, fresh = [
        extended(i, flux[i], push_rows_in, mixed) for i in range(3)
    ]
    push_x = push_x / some_depth
    push_y = push_y / some_depth

    for turn in range(NSUB):
        own = speed_ref if turn == 0 else fast.at[turn - 1]
        diverge = 0.5 * (across(conduct * east) + along(conduct * north))
        wait_fast(turn)
        peak = jnp.maximum(jnp.max(fastest[turn], axis=0), own[...])
        step_dt = courant / jnp.max(peak, axis=1, keepdims=True)
        level = wet * (level + step_dt * (fresh - diverge))
        east, north = (
            wet * (east + step_dt * (rotation * north - 0.5 * across(level) + push_x - friction * east)),
            wet * (north + step_dt * (-rotation * east - 0.5 * along(level) + push_y - friction * north)),
        )
        if turn < NSUB - 1:
            near_east = east[HALO : HALO + nrows, :ncols]
            near_north = north[HALO : HALO + nrows, :ncols]
            speed = root_depth + wet_here * (jnp.abs(near_east) + jnp.abs(near_north))
            fast[turn] = jnp.max(speed, axis=0, keepdims=True)
            send_fast(turn + 1, fast.at[turn])

    for i, value in enumerate((level, east, north)):
        state_ref[i] = value[HALO : HALO + nrows, :ncols]

    for offset in range(1, nc):
        block_copy(offset).wait_send()
    drain_halo(0, *first)
    drain_halo(1, *second)
    for turn in range(NSUB):
        pltpu.make_async_copy(fastest.at[turn], fastest.at[turn], fast_send.at[turn]).wait()


def shards(
    nc, nd,
    atm_fields, send_cols, live_blocks, remap_weights, row_map,
    ocean_depth, wet_mask, sea_level, east_vel, north_vel,
):
    nfield, ncol = atm_fields.shape
    capacity, width = send_cols.shape[3:]
    nrows, ncols = ocean_depth.shape
    f32, bf16 = jnp.float32, jnp.bfloat16
    vmem = pl.BlockSpec(memory_space=pltpu.VMEM)
    smem = pl.BlockSpec(memory_space=pltpu.SMEM)
    anywhere = pl.BlockSpec(memory_space=pl.ANY)

    high = nrows + 2 * HALO
    dma = pltpu.SemaphoreType.DMA
    fluxes, state = pl.pallas_call(
        functools.partial(ocean_kernel, nc, nd),
        name="remap_and_step",
        out_shape=(
            pltpu.VMEM((nfield, nrows, ncols), f32),
            pltpu.VMEM((3, nrows, ncols), f32),
        ),
        in_specs=[vmem, vmem, smem] + [vmem] * 6 + [anywhere],
        out_specs=[vmem, vmem],
        scratch_shapes=[
            pltpu.VMEM((nfield, ncol), f32),
            pltpu.VMEM((nc, capacity * nfield, width), bf16),
            pltpu.VMEM((nc, capacity, width), jnp.int32),
            pltpu.VMEM((5, nrows, ncols), f32),
            pltpu.VMEM((nrows, ncols), f32),
            pltpu.VMEM((1, ncols), f32),
            pltpu.VMEM((nc, capacity, width, width), bf16),
            pltpu.VMEM((nc - 1, capacity * nfield, width), bf16),
            pltpu.VMEM((nfield * nrows // 2, 2 * ncols), f32),
            pltpu.VMEM((nrows, ncols), f32),
            pltpu.VMEM((2, 5, HALO, ncols), f32),
            pltpu.VMEM((2, high, ncols), f32),
            pltpu.VMEM((2, 3, HALO, ncols), f32),
            pltpu.VMEM((2, high, ncols), f32),
            pltpu.VMEM((NSUB - 1, 1, ncols), f32),
            pltpu.VMEM((NSUB, nc * nd - 1, 1, ncols), f32),
            dma((nc,)),
            dma((nc - 1,)),
            dma((nc - 1,)),
            dma((2, 8)),
            dma((2, 8)),
            dma((NSUB,)),
            dma((NSUB,)),
        ],
        compiler_params=pltpu.CompilerParams(collective_id=0, has_side_effects=True),
    )(
        atm_fields, send_cols[0, 0], live_blocks[0, 0], row_map[0, 0],
        ocean_depth, wet_mask, sea_level, east_vel, north_vel, remap_weights[0, 0],
    )
    return pl.pallas_call(
        write_out,
        name="write_out",
        out_shape=(
            jax.ShapeDtypeStruct(fluxes.shape, f32),
            jax.ShapeDtypeStruct(state.shape, f32),
        ),
        in_specs=[vmem, vmem],
        out_specs=[anywhere, anywhere],
        scratch_shapes=[dma((2,))],
        compiler_params=pltpu.CompilerParams(vmem_limit_bytes=4 << 20),
    )(fluxes, state)


def solution(mesh):
    in_specs = (
        P(None, ("comp", "dom")),
        P("comp", "dom", None, None, None),
        P("comp", "dom", None),
        P("comp", "dom", None, None, None, None),
        P("comp", "dom", None, None, None),
        P("dom", "comp"),
        P("dom", "comp"),
        P("dom", "comp"),
        P("dom", "comp"),
        P("dom", "comp"),
    )
    out_specs = (P(None, "dom", "comp"), P(None, "dom", "comp"))
    body = functools.partial(shards, mesh.shape["comp"], mesh.shape["dom"])
    return jax.shard_map(body, mesh=mesh, in_specs=in_specs, out_specs=out_specs, check_vma=False)
```

```python
import functools

import jax
import jax.numpy as jnp
from jax import lax
from jax.experimental import pallas as pl
from jax.experimental.pallas import tpu as pltpu
from jax.sharding import PartitionSpec as P

NSUB = 4
HALO = 2 * NSUB
LANES = 128

courant = 0.5
friction = 0.05

MESH = pl.DeviceIdType.MESH
COMPASS = [(-1, 0), (1, 0), (0, 1), (0, -1), (1, 1), (-1, 1), (1, -1), (-1, -1)]


def nt_dot(a, b):
    return lax.dot_general(a, b, (((1,), (1,)), ((), ())), preferred_element_type=jnp.float32)


def log2(n):
    assert n & (n - 1) == 0
    return n.bit_length() - 1


def pack_edges(fields):
    slot = lax.broadcasted_iota(jnp.int32, fields[0].shape, 1) // (2 * HALO)
    packed = jnp.zeros_like(fields[0])
    for i, field in enumerate(fields):
        packed = jnp.where(slot == i, pltpu.roll(field, 2 * HALO * i + HALO, 1), packed)
    return packed


def write_out(flux_ref, state_ref, flux_out, state_out, sems):
    copies = [
        pltpu.make_async_copy(flux_ref, flux_out, sems.at[0]),
        pltpu.make_async_copy(state_ref, state_out, sems.at[1]),
    ]
    for copy in copies:
        copy.start()
    for copy in copies:
        copy.wait()


def ocean_kernel(
    nc, nd,
    atm_ref, cols_ref, live_ref, map_ref, depth_ref, wet_ref, level_ref, east_ref, north_ref,
    weights_hbm,
    flux, state_ref,
    wide, blocks_ref, target_ref, init_ref, edges_ref, speed_ref,
    weights, arrived, acc, push_edges, rows_in, side_in, push_rows_in, push_side_in,
    fast, fastest,
    weight_sem, block_send, block_recv, halo_send, halo_recv, fast_send, fast_recv,
):
    me_c, me_d = lax.axis_index("comp"), lax.axis_index("dom")
    nfield, nrows, ncols = flux.shape
    capacity, width = target_ref.shape[1:]
    half = nrows // 2
    total = nc * nd

    def weight_copy(offset):
        source = lax.rem(me_c + nc - offset, nc)
        return pltpu.make_async_copy(
            weights_hbm.at[source], weights.at[offset], weight_sem.at[offset]
        )

    def others(act):
        for dc in reversed(range(nc)):
            c = lax.rem(me_c + dc, nc)

            def one(dd, carry, dc=dc, c=c):
                d = lax.rem(me_d + dd, nd)
                act(dc * nd + dd - 1, (c, d))
                return carry

            lower = 1 if dc == 0 else 0
            if nd > 16:
                lax.fori_loop(lower, nd, one, 0)
                continue
            for dd in sorted(range(lower, nd), key=lambda dd: min(dd, nd - dd)):
                one(dd, 0)

    barrier = pltpu.get_barrier_semaphore()
    others(
        lambda slot, device: pl.semaphore_signal(
            barrier, inc=1, device_id=device, device_id_type=MESH
        )
    )
    for offset in range(nc):
        weight_copy(offset).start()

    def send_fast(turn, src):
        def act(slot, device):
            pltpu.make_async_remote_copy(
                src_ref=src,
                dst_ref=fastest.at[turn, slot],
                send_sem=fast_send.at[turn],
                recv_sem=fast_recv.at[turn],
                device_id=device,
                device_id_type=MESH,
            ).start()

        others(act)

    def wait_fast(turn):
        pltpu.make_async_copy(fastest.at[turn], fastest.at[turn], fast_recv.at[turn]).wait()

    def halo_refs(step, rows, edges, rows_into, side_into):
        dr, dc = step
        side = (0 if dc > 0 else 1) if dc else (0 if dr > 0 else 1)
        near = pl.ds(nrows - HALO, HALO) if dr > 0 else pl.ds(0, HALO)
        if dc == 0:
            return rows.at[:, near, :], rows_into.at[side]
        if dr == 0:
            return edges, side_into.at[side, pl.ds(HALO, nrows), :]
        far = pl.ds(0, HALO) if dr > 0 else pl.ds(HALO + nrows, HALO)
        return edges.at[near, :], side_into.at[side, far, :]

    def inside(c, d):
        return (c >= 0) & (c < nc) & (d >= 0) & (d < nd)

    def send_halo(turn, *refs):
        for i, step in enumerate(COMPASS):
            src, dst = halo_refs(step, *refs)
            c, d = me_c + step[1], me_d + step[0]

            @pl.when(inside(c, d))
            def _(i=i, src=src, dst=dst, c=c, d=d):
                pltpu.make_async_remote_copy(
                    src_ref=src,
                    dst_ref=dst,
                    send_sem=halo_send.at[turn, i],
                    recv_sem=halo_recv.at[turn, i],
                    device_id=(c, d),
                    device_id_type=MESH,
                ).start()

    def clear_halo(*refs):
        for step in COMPASS:
            _, dst = halo_refs(step, *refs)

            @pl.when(jnp.logical_not(inside(me_c - step[1], me_d - step[0])))
            def _(dst=dst):
                dst[...] = jnp.zeros(dst.shape, dst.dtype)

    def wait_halo(turn, *refs):
        for i, step in enumerate(COMPASS):
            _, dst = halo_refs(step, *refs)

            @pl.when(inside(me_c - step[1], me_d - step[0]))
            def _(i=i, dst=dst):
                pltpu.make_async_copy(dst, dst, halo_recv.at[turn, i]).wait()

    def drain_halo(turn, *refs):
        for i, step in enumerate(COMPASS):
            src, _ = halo_refs(step, *refs)

            @pl.when(inside(me_c + step[1], me_d + step[0]))
            def _(i=i, src=src):
                pltpu.make_async_copy(src, src, halo_send.at[turn, i]).wait()

    def block_copy(offset):
        peer = lax.rem(me_c + offset, nc)
        return pltpu.make_async_remote_copy(
            src_ref=blocks_ref.at[offset],
            dst_ref=arrived.at[offset - 1],
            send_sem=block_send.at[offset - 1],
            recv_sem=block_recv.at[offset - 1],
            device_id=(peer, me_d),
            device_id_type=MESH,
        )

    wide[...] = atm_ref[...].astype(jnp.float32)
    wetness = wet_ref[...].astype(jnp.float32)
    fields = [level_ref[...], east_ref[...], north_ref[...], depth_ref[...], wetness]
    for i, field in enumerate(fields):
        init_ref[i] = field
    edges_ref[...] = pack_edges(fields)
    speed = jnp.sqrt(fields[3]) + wetness * (jnp.abs(fields[1]) + jnp.abs(fields[2]))
    speed_ref[...] = jnp.max(speed, axis=0, keepdims=True)

    slot = lax.broadcasted_iota(jnp.int32, (capacity, width), 0)
    for s in range(nc):
        target_ref[s] = jnp.where(slot < live_ref[s], map_ref[s], nrows * ncols)

    def gather(offset, carry):
        lists = cols_ref[lax.rem(me_c + offset, nc)]
        for part in range(width // LANES):
            picked = []
            for k in range(capacity):
                index = lists[k : k + 1, part * LANES : (part + 1) * LANES]
                index = jnp.broadcast_to(index, (nfield, LANES))
                high_bits = index >> log2(LANES)
                low_bits = index & (LANES - 1)
                value = jnp.zeros((nfield, LANES), jnp.float32)
                for c in range(wide.shape[1] // LANES):
                    chunk = wide[:, c * LANES : (c + 1) * LANES]
                    taken = jnp.take_along_axis(chunk, low_bits, axis=1, mode="promise_in_bounds")
                    value = jnp.where(high_bits == c, taken, value)
                picked.append(value)
            blocks_ref[offset, :, part * LANES : (part + 1) * LANES] = jnp.concatenate(
                picked, 0
            ).astype(blocks_ref.dtype)
        return carry

    key_iota = lax.broadcasted_iota(jnp.int32, (2 * ncols, width), 0)
    row_iota = lax.broadcasted_iota(jnp.int32, (half, width), 0)

    def spread(values, where_row):
        tall = jnp.broadcast_to(values[:, None, :], (nfield, half, width)).astype(jnp.bfloat16)
        return (tall * where_row[None]).reshape(nfield * half, width)

    def deposit(offset):
        source = lax.rem(me_c + nc - offset, nc)
        blocks = blocks_ref[0] if offset == 0 else arrived[offset - 1]
        targets = target_ref[source]
        tops, rests, keys = [], [], []
        for k in range(capacity):
            product = nt_dot(blocks, weights[offset, k])[k * nfield : (k + 1) * nfield]
            target = targets[k : k + 1, :]
            row = target >> log2(ncols)
            key = ((row >> log2(half)) << log2(ncols)) + (target & (ncols - 1))
            group = row & (half - 1)
            keys.append(jnp.where(key_iota == key, 1.0, 0.0).astype(jnp.bfloat16))
            where_row = jnp.where(row_iota == group, 1.0, 0.0).astype(jnp.bfloat16)
            top = product.astype(jnp.bfloat16).astype(jnp.float32)
            tops.append(spread(top, where_row))
            rests.append(spread(product - top, where_row))
        update = nt_dot(jnp.concatenate(tops + rests, 1), jnp.concatenate(keys + keys, 1))
        if offset == 0:
            acc[...] = update
        else:
            acc[...] += update

    first = (init_ref, edges_ref, rows_in, side_in)
    second = (flux.at[pl.ds(0, 3)], push_edges, push_rows_in, push_side_in)
    clear_halo(*first)
    clear_halo(*second)
    lax.fori_loop(0, nc, gather, 0)

    pl.semaphore_wait(barrier, total - 1)
    for offset in range(1, nc):
        block_copy(offset).start()
    send_halo(0, *first)
    send_fast(0, speed_ref)

    for offset in range(nc):
        weight_copy(offset).wait()
        if offset:
            block_copy(offset).wait_recv()
        deposit(offset)

    pushes = []
    for f in range(nfield):
        upper = acc[f * half : (f + 1) * half, :ncols]
        lower = acc[f * half : (f + 1) * half, ncols:]
        flux[f, :half] = upper
        flux[f, half:] = lower
        if f < 3:
            pushes.append(jnp.concatenate([upper, lower], 0))
        if f == 2:
            push_edges[...] = pack_edges(pushes)
    send_halo(1, *second)

    high = nrows + 2 * HALO
    lane = lax.broadcasted_iota(jnp.int32, (high, ncols), 1)
    beside = (lane < HALO) | (lane >= ncols - HALO)
    west_part = (lane & (2 * HALO - 1)) < HALO

    def extended(i, center, rows, mixed):
        main = jnp.concatenate([rows[0, i], center, rows[1, i]], 0)
        side = pltpu.roll(mixed, ncols - (2 * HALO * i + HALO), 1)
        return jnp.concatenate([main, jnp.where(beside, side, 0.0)], 1)

    wait_halo(0, *first)
    mixed = jnp.where(west_part, side_in[0], side_in[1])
    level, east, north, depth, wet = [
        extended(i, init_ref[i], rows_in, mixed) for i in range(5)
    ]
    root_depth = jnp.sqrt(init_ref[3])
    wet_here = init_ref[4]
    conduct = depth * wet
    some_depth = jnp.where(depth > 0.0, depth, 1.0)
    global_row = (
        lax.broadcasted_iota(jnp.int32, (high, 2 * ncols), 0) + (me_d * nrows - HALO)
    ).astype(jnp.float32)
    rotation = 0.1 + 0.4 * (global_row + 0.5) / (nrows * nd)

    def across(x):
        return pltpu.roll(x, 2 * ncols - 1, 1) - pltpu.roll(x, 1, 1)

    def along(x):
        return pltpu.roll(x, high - 1, 0) - pltpu.roll(x, 1, 0)

    wait_halo(1, *second)
    mixed = jnp.where(west_part, push_side_in[0], push_side_in[1])
    push_x, push_y, fresh = [
        extended(i, flux[i], push_rows_in, mixed) for i in range(3)
    ]
    push_x = push_x / some_depth
    push_y = push_y / some_depth

    for turn in range(NSUB):
        own = speed_ref if turn == 0 else fast.at[turn - 1]
        diverge = 0.5 * (across(conduct * east) + along(conduct * north))
        still, rise = wet * level, wet * (fresh - diverge)
        pull_x = rotation * north - 0.5 * across(still) + push_x - friction * east
        pull_y = -rotation * east - 0.5 * along(still) + push_y - friction * north
        slope_x, slope_y = 0.5 * across(rise), 0.5 * along(rise)
        wait_fast(turn)
        peak = jnp.maximum(jnp.max(fastest[turn], axis=0), own[...])
        step_dt = courant / jnp.max(peak, axis=1, keepdims=True)
        level = still + step_dt * rise
        east = wet * (east + step_dt * (pull_x - step_dt * slope_x))
        north = wet * (north + step_dt * (pull_y - step_dt * slope_y))
        if turn < NSUB - 1:
            near_east = east[HALO : HALO + nrows, :ncols]
            near_north = north[HALO : HALO + nrows, :ncols]
            speed = root_depth + wet_here * (jnp.abs(near_east) + jnp.abs(near_north))
            fast[turn] = jnp.max(speed, axis=0, keepdims=True)
            send_fast(turn + 1, fast.at[turn])

    for i, value in enumerate((level, east, north)):
        state_ref[i] = value[HALO : HALO + nrows, :ncols]

    for offset in range(1, nc):
        block_copy(offset).wait_send()
    drain_halo(0, *first)
    drain_halo(1, *second)
    for turn in range(NSUB):
        pltpu.make_async_copy(fastest.at[turn], fastest.at[turn], fast_send.at[turn]).wait()


def shards(
    nc, nd,
    atm_fields, send_cols, live_blocks, remap_weights, row_map,
    ocean_depth, wet_mask, sea_level, east_vel, north_vel,
):
    nfield, ncol = atm_fields.shape
    capacity, width = send_cols.shape[3:]
    nrows, ncols = ocean_depth.shape
    f32, bf16 = jnp.float32, jnp.bfloat16
    vmem = pl.BlockSpec(memory_space=pltpu.VMEM)
    smem = pl.BlockSpec(memory_space=pltpu.SMEM)
    anywhere = pl.BlockSpec(memory_space=pl.ANY)

    high = nrows + 2 * HALO
    dma = pltpu.SemaphoreType.DMA
    fluxes, state = pl.pallas_call(
        functools.partial(ocean_kernel, nc, nd),
        name="remap_and_step",
        out_shape=(
            pltpu.VMEM((nfield, nrows, ncols), f32),
            pltpu.VMEM((3, nrows, ncols), f32),
        ),
        in_specs=[vmem, vmem, smem] + [vmem] * 6 + [anywhere],
        out_specs=[vmem, vmem],
        scratch_shapes=[
            pltpu.VMEM((nfield, ncol), f32),
            pltpu.VMEM((nc, capacity * nfield, width), bf16),
            pltpu.VMEM((nc, capacity, width), jnp.int32),
            pltpu.VMEM((5, nrows, ncols), f32),
            pltpu.VMEM((nrows, ncols), f32),
            pltpu.VMEM((1, ncols), f32),
            pltpu.VMEM((nc, capacity, width, width), bf16),
            pltpu.VMEM((nc - 1, capacity * nfield, width), bf16),
            pltpu.VMEM((nfield * nrows // 2, 2 * ncols), f32),
            pltpu.VMEM((nrows, ncols), f32),
            pltpu.VMEM((2, 5, HALO, ncols), f32),
            pltpu.VMEM((2, high, ncols), f32),
            pltpu.VMEM((2, 3, HALO, ncols), f32),
            pltpu.VMEM((2, high, ncols), f32),
            pltpu.VMEM((NSUB - 1, 1, ncols), f32),
            pltpu.VMEM((NSUB, nc * nd - 1, 1, ncols), f32),
            dma((nc,)),
            dma((nc - 1,)),
            dma((nc - 1,)),
            dma((2, 8)),
            dma((2, 8)),
            dma((NSUB,)),
            dma((NSUB,)),
        ],
        compiler_params=pltpu.CompilerParams(collective_id=0, has_side_effects=True),
    )(
        atm_fields, send_cols[0, 0], live_blocks[0, 0], row_map[0, 0],
        ocean_depth, wet_mask, sea_level, east_vel, north_vel, remap_weights[0, 0],
    )
    return pl.pallas_call(
        write_out,
        name="write_out",
        out_shape=(
            jax.ShapeDtypeStruct(fluxes.shape, f32),
            jax.ShapeDtypeStruct(state.shape, f32),
        ),
        in_specs=[vmem, vmem],
        out_specs=[anywhere, anywhere],
        scratch_shapes=[dma((2,))],
        compiler_params=pltpu.CompilerParams(vmem_limit_bytes=4 << 20),
    )(fluxes, state)


def solution(mesh):
    in_specs = (
        P(None, ("comp", "dom")),
        P("comp", "dom", None, None, None),
        P("comp", "dom", None),
        P("comp", "dom", None, None, None, None),
        P("comp", "dom", None, None, None),
        P("dom", "comp"),
        P("dom", "comp"),
        P("dom", "comp"),
        P("dom", "comp"),
        P("dom", "comp"),
    )
    out_specs = (P(None, "dom", "comp"), P(None, "dom", "comp"))
    body = functools.partial(shards, mesh.shape["comp"], mesh.shape["dom"])
    return jax.shard_map(body, mesh=mesh, in_specs=in_specs, out_specs=out_specs, check_vma=False)
```
